32 devices in a mesh: member: 2 (over y), seq: 4 (over z), dp: 2 (over x), mp: 2 (over core).
Axes of the slice: x: 2, y: 2, z: 4, core: 2. Of those that a mesh axis runs over, the one named last changes fastest.
Arguments:
- mixer_in: bfloat16 [4, 512, 3072], P(('member', 'dp'), 'seq', 'mp'), parts along dimension 0, may hold values from -6 to 6
- delta_raw: bfloat16 [4, 512, 3072], P(('member', 'dp'), 'seq', 'mp'), parts along dimension 0, may hold values from -2 to 512
- delta_bias: float32 [6144], P(('member', 'mp')), parts along dimension 0, may hold values from -4 to -2
- decay_log: float32 [6144, 16], P(('member', 'mp')), parts along dimension 0, may hold values from -12 to 1
- skip_gain: float32 [6144], P(('member', 'mp')), parts along dimension 0, may hold values from 0.5 to 1.5
- state_write: bfloat16 [4, 512, 16], P(('member', 'dp'), 'seq'), parts along dimension 0, may hold values from -5 to 5
- state_read: bfloat16 [4, 512, 16], P(('member', 'dp'), 'seq'), parts along dimension 0, may hold values from -1.5 to 1.5
- mixer_grad: bfloat16 [4, 512, 3072], P(('member', 'dp'), 'seq', 'mp'), parts along dimension 0, may hold values from -6 to 6
- attn_query: bfloat16 [4, 512, 1536], P(('member', 'dp'), 'seq', 'mp'), parts along dimension 0, may hold values from -5 to 5
- attn_key: bfloat16 [4, 512, 1536], P(('member', 'dp'), 'seq', 'mp'), parts along dimension 0, may hold values from -5 to 5
- attn_value: bfloat16 [4, 512, 1536], P(('member', 'dp'), 'seq', 'mp'), parts along dimension 0, may hold values from -6 to 6
- attn_grad: bfloat16 [4, 512, 1536], P(('member', 'dp'), 'seq', 'mp'), parts along dimension 0, may hold values from -6 to 6
- document_id: int32 [4, 512], P(('member', 'dp'), 'seq'), parts along dimension 0, may hold values from 0 to 3, never falling along the last dimension, each value on 1 to 256 neighbouring positions
Outputs:
- mixer_out: bfloat16 [4, 512, 3072], P(('member', 'dp'), 'seq', 'mp'), parts along dimension 0
- input_grad: bfloat16 [4, 512, 3072], P(('member', 'dp'), 'seq', 'mp'), parts along dimension 0
- delta_grad: bfloat16 [4, 512, 3072], P(('member', 'dp'), 'seq', 'mp'), parts along dimension 0
- decay_grad: float32 [6144, 16], P(('member', 'mp')), parts along dimension 0
- skip_grad: float32 [6144], P(('member', 'mp')), parts along dimension 0
- bias_grad: float32 [6144], P(('member', 'mp')), parts along dimension 0
- attn_out: bfloat16 [4, 512, 1536], P(('member', 'dp'), 'seq', 'mp'), parts along dimension 0
- query_grad: bfloat16 [4, 512, 1536], P(('member', 'dp'), 'seq', 'mp'), parts along dimension 0
- key_grad: bfloat16 [4, 512, 1536], P(('member', 'dp'), 'seq', 'mp'), parts along dimension 0
- value_grad: bfloat16 [4, 512, 1536], P(('member', 'dp'), 'seq', 'mp'), parts along dimension 0
The draws below stay inside these ranges and needn't reach their ends.
There are 2 independent parts, one for each index of `member`. The reference program is written for one: setup_inputs(seed, part) draws one part's arguments, and reference() takes and returns one part's arrays. A program takes and returns all parts, laid end to end along the dimension named above; each array names one. Nothing has to cross between parts.
Inputs may be any that keep to these rules, and one draw needn't show every extreme that they name: `document_id`: document numbers never fall along a sequence; a document covers at most 256 positions.
All inputs are finite; a program needn't handle non-finite values.
Results may differ from the reference program's by a relative error of at most 0.024.
Values may be sent and summed in bfloat16 or wider, within the bound.
A program may use at most 128 MiB of HBM per device.

```python
import math
import jax
import jax.numpy as jnp
import numpy as np
from jax import lax

CH = 3072
STATE = 16
HEADS = 16
HD = 96
DOCS = 4
TOK_DEV = 128
SEQ = 512
BATCH = 2
WINDOW = 128


def mamba_law(key):
    base = jax.random.fold_in(key, 23)
    parts = jax.random.split(base, 10)
    fast_share = 0.5
    is_fast = jax.random.uniform(parts[0], (CH,)) < fast_share
    fast_rate = jnp.exp(jax.random.uniform(parts[1], (CH,), jnp.float32, math.log(1.0 / 50.0), math.log(1.0 / 30.0)))
    slow_rate = jnp.exp(jax.random.uniform(parts[2], (CH,), jnp.float32, math.log(0.3 / SEQ), math.log(0.9 / SEQ)))
    rate = jnp.where(is_fast, fast_rate, slow_rate)
    base_step = jnp.exp(jax.random.uniform(parts[3], (CH,), jnp.float32, math.log(0.025), math.log(0.1)))
    offset_bias = jnp.log(jnp.expm1(base_step))
    spread = jnp.exp(jax.random.uniform(parts[4], (CH, STATE), jnp.float32, -0.35, 0.35))
    absolute_size = (rate / base_step)[:, None] * spread
    noise = 0.3 * jnp.clip(jax.random.normal(parts[5], (BATCH, SEQ, CH), jnp.float32), -4.0, 4.0)
    regions = jax.random.uniform(parts[6], (BATCH, SEQ // TOK_DEV, 1, CH), jnp.float32, -0.7, 0.7)
    noise = noise + jnp.broadcast_to(regions, (BATCH, SEQ // TOK_DEV, TOK_DEV, CH)).reshape(BATCH, SEQ, CH)
    places = jax.random.randint(parts[7], (BATCH, 3), 0, SEQ)
    objective_value = jax.random.uniform(parts[8], (BATCH, 3), jnp.float32, 0.25, 0.5)
    matched_flag = (places[:, :, None] == jnp.arange(SEQ)[None, None, :]).astype(jnp.float32)
    spike_step_size = (-jnp.log1p(-objective_value))[:, :, None] / jnp.mean(absolute_size, axis=1)[None, None, :]
    spike_raw_values = spike_step_size + jnp.log1p(-jnp.exp(-spike_step_size)) - offset_bias[None, None, :]
    any_hit = jnp.sum(matched_flag, axis=1) > 0.5
    selected_entries = jnp.einsum('ltv,lte->lve', matched_flag, spike_raw_values)
    raw = jnp.where(any_hit[:, :, None], selected_entries, noise)
    write = jnp.clip(jax.random.normal(parts[9], (BATCH, SEQ, STATE), jnp.float32), -5.0, 5.0)
    write = write * jnp.where(any_hit, 0.01, 1.0)[:, :, None]
    return (offset_bias, jnp.log(absolute_size), raw, write)


def attention_law(key):
    base = jax.random.fold_in(key, 41)
    parts = jax.random.split(base, 2)
    width = HEADS * HD
    query = jnp.clip(jax.random.normal(parts[0], (BATCH, SEQ, width), jnp.float32), -5.0, 5.0)
    keyset = jnp.clip(jax.random.normal(parts[1], (BATCH, SEQ, width), jnp.float32), -5.0, 5.0)
    return (query, keyset)


def draw_delta_raw(key, part):
    return mamba_law(key)[2].astype(jnp.bfloat16)


def draw_delta_bias(key, part):
    return mamba_law(key)[0].astype(jnp.float32)


def draw_decay_log(key, part):
    return mamba_law(key)[1].astype(jnp.float32)


def draw_state_write(key, part):
    return mamba_law(key)[3].astype(jnp.bfloat16)


def draw_attn_query(key, part):
    return attention_law(key)[0].astype(jnp.bfloat16)


def draw_attn_key(key, part):
    return attention_law(key)[1].astype(jnp.bfloat16)


def level_of(key, dims, cuts, least, high):
    level = 1.0
    for position, shards_of in cuts:
        heights = jax.random.uniform(jax.random.fold_in(jax.random.fold_in(key, 6), position), (shards_of,), jnp.float32, least / len(cuts), high / len(cuts))
        level = level * jnp.repeat(jnp.exp(heights), dims[position] // shards_of).reshape((-1,) + (1,) * (len(dims) - 1 - position))
    return level


def length_profile(count, total, limit, slope):
    loads = [(1 << 20) // math.isqrt(rank ** slope) + 1 for rank in range(2, count + 1)]
    spare, holding = total - limit - (count - 1), [1] * (count - 1)
    while spare > 0:
        movable = [i for i in range(count - 1) if holding[i] < limit]
        whole, remaining = sum([loads[i] for i in movable]), spare
        for i in movable:
            more = min(limit - holding[i], max(1, remaining * loads[i] // whole), spare)
            holding[i] = holding[i] + more
            spare = spare - more
    return np.array([limit] + holding)


def uneven(rng, amount, total, most, slope):
    if amount == 2:
        one = jax.random.randint(rng, (), max(1, total - most), min(most, total - 1) + 1)
        return jnp.stack([one, total - one])
    tallies = jnp.asarray(length_profile(amount, total, most, slope), jnp.int32)
    pairs = (amount - 1) // 2
    donor, receiver = tallies[1:1 + 2 * pairs:2], tallies[2:2 + 2 * pairs:2]
    margin = jnp.minimum(donor - 1, most - receiver)
    moved = jax.random.randint(jax.random.fold_in(rng, 1), (pairs,), 0, 1 << 20) % (margin + 1)
    tallies = tallies.at[1:1 + 2 * pairs:2].set(donor - moved).at[2:2 + 2 * pairs:2].set(receiver + moved)
    return tallies[jax.random.permutation(jax.random.fold_in(rng, 2), amount)]


def scatter_about(rng, shape, scale, bound, shards=(), dtype=jnp.bfloat16):
    result = jax.random.normal(rng, shape, jnp.float32) * scale
    if len(shards) > 0:
        result = level_of(rng, shape, shards, -0.22, 0.18) * result
    return jnp.clip(result, min=-bound, max=bound).astype(dtype)


def setup_inputs(seed: int = 0, part: int = 0) -> dict:
    key_of = jax.random.split(jax.random.key(seed), 14)
    part_splits = jax.random.split(jax.random.fold_in(key_of[13], part), 14)
    return {
        "mixer_in": scatter_about(part_splits[0], (BATCH, SEQ, CH), 1.0, 6.0, ((0, 2), (1, 4), (2, 2))),
        "delta_raw": draw_delta_raw(jax.random.fold_in(jax.random.fold_in(key_of[13], part), 71), part),
        "delta_bias": draw_delta_bias(jax.random.fold_in(jax.random.fold_in(key_of[13], part), 71), part),
        "decay_log": draw_decay_log(jax.random.fold_in(jax.random.fold_in(key_of[13], part), 71), part),
        "skip_gain": jnp.clip(1.0 + 0.1 * jax.random.normal(part_splits[4], (CH,), jnp.float32), 0.5, 1.5),
        "state_write": draw_state_write(jax.random.fold_in(jax.random.fold_in(key_of[13], part), 71), part),
        "state_read": scatter_about(part_splits[6], (BATCH, SEQ, STATE), 0.25, 1.5, ((0, 2), (1, 4))),
        "mixer_grad": scatter_about(part_splits[7], (BATCH, SEQ, CH), 1.0, 6.0, ((0, 2), (1, 4), (2, 2))),
        "attn_query": draw_attn_query(jax.random.fold_in(jax.random.fold_in(key_of[13], part), 71), part),
        "attn_key": draw_attn_key(jax.random.fold_in(jax.random.fold_in(key_of[13], part), 71), part),
        "attn_value": scatter_about(part_splits[10], (BATCH, SEQ, HEADS * HD), 1.0, 6.0, ((0, 2), (1, 4), (2, 2))),
        "attn_grad": scatter_about(part_splits[11], (BATCH, SEQ, HEADS * HD), 1.0, 6.0, ((0, 2), (1, 4), (2, 2))),
        "document_id": jax.vmap(lambda own: jnp.searchsorted(jnp.cumsum(uneven(own, DOCS, SEQ, SEQ // 2, 0)), jnp.arange(SEQ), side="right"))(jax.random.split(part_splits[12], BATCH)).reshape((BATCH, SEQ)).astype(jnp.int32),
    }


def mamba_group(inputs, raws, grads, writes, reads, decay_log, skip, offset_bias):
    step_size = jax.nn.softplus(raws + offset_bias[None, :])
    rate = -jnp.exp(decay_log)
    weighted = step_size * inputs
    start = jnp.zeros(rate.shape, jnp.float32)

    def advance(state, items):
        sizes, weights, write_row = items
        state = jnp.exp(sizes[:, None] * rate) * state + weights[:, None] * write_row[None, :]
        return (state, state)
    _, states = lax.scan(advance, start, (step_size, weighted, writes))
    mixed = jnp.einsum('ten,tn->te', states, reads, precision=lax.Precision.HIGHEST) + skip[None, :] * inputs
    previous = jnp.concatenate([start[None], states[:-1]], axis=0)

    def retreat(carry, items):
        back, accum = carry
        sizes, values, outs, write_row, read_row, prior = items
        decay = jnp.exp(sizes[:, None] * rate)
        adjoint = read_row[None, :] * outs[:, None] + back
        through_write = lax.optimization_barrier(jnp.sum(adjoint * write_row[None, :], axis=1))
        input_part = through_write * sizes + skip * outs
        tail = adjoint * prior * decay
        step_part = values * through_write + lax.optimization_barrier(jnp.sum(tail * rate, axis=1))
        accum = accum + tail * sizes[:, None]
        return ((decay * adjoint, accum), (input_part, step_part))
    (_, accum), (input_grad, step_grad) = lax.scan(retreat, (start, start), (step_size, inputs, grads, writes, reads, previous), reverse=True)
    raw_grad = step_grad * jax.nn.sigmoid(raws + offset_bias[None, :])
    return (mixed, input_grad, raw_grad, accum * rate, lax.optimization_barrier(jnp.sum(grads * inputs, axis=0)), lax.optimization_barrier(jnp.sum(raw_grad, axis=0)))

def attend_block(items):
    query, key_now, key_before, value_now, value_before, out_grad, doc_now, doc_before = items
    length = query.shape[0]
    width = query.shape[1]
    heads = width // HD
    key_all = jnp.concatenate([key_before, key_now], axis=0).reshape(2 * length, heads, HD).astype(jnp.float32)
    value_all = jnp.concatenate([value_before, value_now], axis=0).reshape(2 * length, heads, HD).astype(jnp.float32)
    doc_all = jnp.concatenate([doc_before, doc_now], axis=0)
    query_heads = query.reshape(length, heads, HD).astype(jnp.float32)
    grad_heads = out_grad.reshape(length, heads, HD).astype(jnp.float32)
    offset = jnp.arange(length)[:, None] + length - jnp.arange(2 * length)[None, :]
    allowed = (offset >= 0) & (offset < WINDOW) & (doc_all[None, :] == doc_now[:, None])
    scale = 1.0 / math.sqrt(HD)
    scores = jnp.einsum('qhd,khd->hqk', query_heads, key_all) * scale
    scores = jnp.where(allowed[None], scores, -1e+30)
    top = lax.optimization_barrier(jnp.max(scores, axis=2))
    total = top + jnp.log(lax.optimization_barrier(jnp.sum(jnp.exp(scores - top[:, :, None]), axis=2)))
    probs = jnp.exp(scores - total[:, :, None])
    probs_low = lax.optimization_barrier(probs.astype(jnp.bfloat16)).astype(jnp.float32)
    attended = jnp.einsum('hqk,khd->qhd', probs_low, value_all).astype(jnp.bfloat16)
    attended_wide = lax.optimization_barrier(attended).astype(jnp.float32)
    row_term = jnp.einsum('qhd,qhd->hq', grad_heads, attended_wide)
    value_score = jnp.einsum('qhd,khd->hqk', grad_heads, value_all)
    score_grad = lax.optimization_barrier((probs * (value_score - row_term[:, :, None])).astype(jnp.bfloat16)).astype(jnp.float32)
    query_grad = (jnp.einsum('hqk,khd->qhd', score_grad, key_all) * scale).astype(jnp.bfloat16)
    key_parts = jnp.einsum('hqk,qhd->khd', score_grad, query_heads) * scale
    value_parts = jnp.einsum('hqk,qhd->khd', probs_low, grad_heads)
    return (attended.reshape(length, width), query_grad.reshape(length, width), key_parts.reshape(2 * length, width), value_parts.reshape(2 * length, width))

def reference(mixer_in, delta_raw, delta_bias, decay_log, skip_gain, state_write, state_read, mixer_grad, attn_query, attn_key, attn_value, attn_grad, document_id):
    group = math.gcd(CH, 512)
    groups = CH // group

    def split_channels(values):
        return values.reshape(SEQ, groups, group).transpose(1, 0, 2)

    def merge_channels(values):
        return values.transpose(1, 0, 2).reshape(SEQ, CH)

    def one_row(items):
        inputs, raws, grads, writes, reads = items
        pieces = (split_channels(inputs), split_channels(raws), split_channels(grads), decay_log.reshape(groups, group, STATE), skip_gain.reshape(groups, group), delta_bias.reshape(groups, group))

        def one_group(piece):
            return mamba_group(piece[0], piece[1], piece[2], writes, reads, piece[3], piece[4], piece[5])
        outs = lax.map(one_group, pieces)
        return (merge_channels(outs[0]).astype(jnp.bfloat16), merge_channels(outs[1]).astype(jnp.bfloat16), merge_channels(outs[2]).astype(jnp.bfloat16), outs[3].reshape(CH, STATE), outs[4].reshape(CH), outs[5].reshape(CH))
    rows = lax.map(one_row, (mixer_in.astype(jnp.float32), delta_raw.astype(jnp.float32), mixer_grad.astype(jnp.float32), state_write.astype(jnp.float32), state_read.astype(jnp.float32)))
    scale = 1.0 / math.sqrt(BATCH * SEQ)
    decay_grad = lax.optimization_barrier(jnp.sum(rows[3], axis=0)) * scale
    skip_grad = lax.optimization_barrier(jnp.sum(rows[4], axis=0)) * scale
    bias_grad = lax.optimization_barrier(jnp.sum(rows[5], axis=0)) * scale
    blocks = SEQ // TOK_DEV
    width = HEADS * HD

    def to_blocks(values):
        return values.reshape(BATCH, blocks, TOK_DEV, width)

    def earlier(values):
        return jnp.concatenate([jnp.zeros_like(values[:, :1]), values[:, :-1]], axis=1)

    def flat(values):
        return values.reshape((BATCH * blocks,) + values.shape[2:])
    query_b = to_blocks(attn_query)
    key_b = to_blocks(attn_key)
    value_b = to_blocks(attn_value)
    grad_b = to_blocks(attn_grad)
    docs = document_id.reshape(BATCH, blocks, TOK_DEV).astype(jnp.int32)
    doc_prev = jnp.concatenate([jnp.full((BATCH, 1, TOK_DEV), -1, jnp.int32), docs[:, :-1]], axis=1)
    outs = lax.map(attend_block, (flat(query_b), flat(key_b), flat(earlier(key_b)), flat(value_b), flat(earlier(value_b)), flat(grad_b), flat(docs), flat(doc_prev)))
    attended = outs[0].reshape(BATCH, SEQ, width)
    query_grad = outs[1].reshape(BATCH, SEQ, width)
    key_parts = outs[2].reshape(BATCH, blocks, 2 * TOK_DEV, width)
    value_parts = outs[3].reshape(BATCH, blocks, 2 * TOK_DEV, width)

    def combine(parts):
        own = parts[:, :, TOK_DEV:]
        before = parts[:, :, :TOK_DEV]
        later = jnp.concatenate([before[:, 1:], jnp.zeros_like(before[:, :1])], axis=1)
        return (own + later).astype(jnp.bfloat16).reshape(BATCH, SEQ, width)
    return (rows[0], rows[1], rows[2], decay_grad, skip_grad, bias_grad, attended, query_grad, combine(key_parts), combine(value_parts))
```

```python
import functools
import math

import jax
import jax.numpy as jnp
from jax import lax
from jax.experimental import pallas as pl
from jax.experimental.pallas import tpu as pltpu
from jax.sharding import PartitionSpec as P

HD = 96
WINDOW = 128
LANES = 128
SUB = 8
RED_ROWS = 24
LOG2E = math.log2(math.e)
LN2 = math.log(2.0)
NEG = -1e30
MESH = pl.DeviceIdType.MESH


def dot(a, b, contract):
    return lax.dot_general(a, b, (contract, ((), ())), preferred_element_type=jnp.float32)


def nn(a, b):
    return dot(a, b, ((1,), (0,)))


def nt(a, b):
    return dot(a, b, ((1,), (1,)))


def tn(a, b):
    return dot(a, b, ((0,), (0,)))


def kernel(
    shards,
    copies,
    x_ref, raw_ref, grad_ref, bias_ref, decay_ref, skip_ref, write_ref, read_ref,
    q_ref, k_ref, v_ref, do_ref, doc_ref,
    mix_ref, xgrad_ref, rgrad_ref, sums_ref, att_ref, qgrad_ref, kgrad_ref, vgrad_ref,
    xp, gp, step, sig, wb, rb, rate2, ends, through, leads,
    dev_end, dev_through, dev_lead, state_in, adj_in, state_out, adj_out,
    dec, prev, fold, mix_p, xg_p, rg_p,
    k_prev, v_prev, q_next, do_next, doc_prev, doc_next,
    stats, stats_next, key_own, value_own, mask_prev, mask_now, mask_next,
    red, rs_buf, fin,
    near_send, near_recv, chain_send, chain_recv, rs_send, rs_recv, ag_send, ag_recv,
):
    z, dp = lax.axis_index("seq"), lax.axis_index("dp")
    peers = shards * copies
    me = dp * shards + z
    length, channels = x_ref.shape
    states = decay_ref.shape[0]
    blocks = channels // LANES
    steps = length // SUB
    heads = q_ref.shape[1] // HD
    slots = rs_buf.shape[0]

    def at(peer):
        return {"seq": peer % shards, "dp": peer // shards}

    barrier = pltpu.get_barrier_semaphore()

    def greet(peer, carry):
        @pl.when(peer != me)
        def _():
            pl.semaphore_signal(barrier, inc=1, device_id=at(peer), device_id_type=MESH)

        return carry

    lax.fori_loop(0, peers, greet, 0)
    pl.semaphore_wait(barrier, peers - 1)

    def near(index, src, dst, offset, sems=None):
        send, recv = sems or (near_send, near_recv)
        return pltpu.make_async_remote_copy(
            src_ref=src,
            dst_ref=dst,
            send_sem=send.at[index],
            recv_sem=recv.at[index],
            device_id={"seq": z + offset},
            device_id_type=MESH,
        )

    up = [near(0, doc_ref, doc_prev, 1), near(1, k_ref, k_prev, 1), near(2, v_ref, v_prev, 1)]
    down = [
        near(3, doc_ref, doc_next, -1),
        near(4, q_ref, q_next, -1),
        near(5, do_ref, do_next, -1),
    ]
    stats_copy = near(6, stats, stats_next, -1)
    chain = (chain_send, chain_recv)
    state_copy = near(0, state_out, state_in, 1, chain)
    adj_copy = near(1, adj_out, adj_in, -1, chain)

    @pl.when(z < shards - 1)
    def _():
        for copy in up:
            copy.start()

    @pl.when(z > 0)
    def _():
        for copy in down:
            copy.start()

    @pl.when(z == 0)
    def _():
        k_prev[...] = jnp.zeros_like(k_prev)
        v_prev[...] = jnp.zeros_like(v_prev)
        doc_prev[...] = jnp.zeros_like(doc_prev)
        state_in[...] = jnp.zeros_like(state_in)

    @pl.when(z == shards - 1)
    def _():
        q_next[...] = jnp.zeros_like(q_next)
        do_next[...] = jnp.zeros_like(do_next)
        doc_next[...] = jnp.zeros_like(doc_next)
        stats_next[...] = jnp.zeros_like(stats_next)
        adj_in[...] = jnp.zeros_like(adj_in)

    row = lax.broadcasted_iota(jnp.int32, (length, length), 0)
    col = lax.broadcasted_iota(jnp.int32, (length, length), 1)
    order = (col == steps * (row % SUB) + row // SUB).astype(jnp.float32).astype(jnp.bfloat16)
    back_order = (row == steps * (col % SUB) + col // SUB).astype(jnp.float32).astype(jnp.bfloat16)

    writes = nn(order, write_ref[...])
    reads = nn(order, read_ref[...])
    for n in range(states):
        wb[0, :, n] = jnp.broadcast_to(writes[:, n : n + 1], (length, LANES)).reshape(
            steps, SUB, LANES
        )
        wb[1, :, n] = jnp.broadcast_to(reads[:, n : n + 1], (length, LANES)).reshape(
            steps, SUB, LANES
        )
    rate2[...] = -jnp.exp(decay_ref[...]) * LOG2E

    def lanes_of(b):
        return pl.ds(pl.multiple_of(b * LANES, LANES), LANES)

    half = states // 2

    def first_pass(b, carry):
        lanes = lanes_of(b)
        xp[:, lanes] = nn(order, x_ref[:, lanes])
        gp[:, lanes] = nn(order, grad_ref[:, lanes])
        arg = nn(order, raw_ref[:, lanes]) + bias_ref[:, lanes]
        small = jnp.exp(-jnp.abs(arg))
        step[:, lanes] = jnp.maximum(arg, 0.0) + jnp.log(1.0 + small)
        sig[:, lanes] = jnp.where(arg >= 0.0, 1.0, small) / (1.0 + small)
        rates = rate2[:, lanes]
        for n in range(states):
            rb[b, n] = jnp.broadcast_to(rates[n : n + 1], (SUB, LANES))
        for part in range(2):
            some = pl.ds(part * half, half)
            rate = rb[b, some]
            state = jnp.zeros((half, SUB, LANES), jnp.float32)
            lead = jnp.zeros((half, SUB, LANES), jnp.float32)
            product = None
            for s in range(steps):
                rows = pl.ds(s * SUB, SUB)
                size = step[rows, lanes]
                weight = size * xp[rows, lanes]
                decay = jnp.exp2(size[None] * rate)
                state = decay * state + weight[None] * wb[0, s, some]
                product = decay if product is None else product * decay
                lead = lead + product * (gp[rows, lanes][None] * wb[1, s, some])
            flat = pl.ds(part * half * SUB, half * SUB)
            ends[b, flat] = state.reshape(half * SUB, LANES)
            through[b, flat] = product.reshape(half * SUB, LANES)
            leads[b, flat] = lead.reshape(half * SUB, LANES)
        end = jnp.zeros((states, LANES), jnp.float32)
        lead = jnp.zeros((states, LANES), jnp.float32)
        total = jnp.ones((states, LANES), jnp.float32)
        for j in range(SUB):
            rows = pl.ds(j, states, stride=SUB)
            now = through[b, rows]
            end = ends[b, rows] + now * end
            total = total * now
            rows = pl.ds(SUB - 1 - j, states, stride=SUB)
            lead = leads[b, rows] + through[b, rows] * lead
        dev_end[:, lanes] = end
        dev_lead[:, lanes] = lead
        dev_through[:, lanes] = total
        return carry

    lax.fori_loop(0, blocks, first_pass, 0)

    def hop(k):
        @pl.when(z == k)
        def _():
            if k > 0:
                state_copy.wait_recv()
            if k < shards - 1:
                state_out[...] = dev_end[...] + dev_through[...] * state_in[...]
                state_copy.start()

        @pl.when(z == shards - 1 - k)
        def _():
            if k > 0:
                adj_copy.wait_recv()
            if k < shards - 1:
                adj_out[...] = dev_lead[...] + dev_through[...] * adj_in[...]
                adj_copy.start()

    hop(0)

    @pl.when(z > 0)
    def _():
        for copy in up:
            copy.wait_recv()

    docs_now = jnp.broadcast_to(doc_ref[...].astype(jnp.float32), (length, length))
    docs_prev = jnp.broadcast_to(doc_prev[...].astype(jnp.float32), (length, length))
    docs_own = docs_now.T
    seen = (docs_now == docs_own) & (row >= col)
    mask_now[...] = jnp.where(seen, 0.0, NEG)
    seen = (docs_prev == docs_own) & (row < col) & (z > 0)
    mask_prev[...] = jnp.where(seen, 0.0, NEG)
    scale = 1.0 / math.sqrt(HD)

    def head_first(h):
        span = pl.ds(h * HD, HD)
        q, k, v, do = q_ref[:, span], k_ref[:, span], v_ref[:, span], do_ref[:, span]
        kb, vb = k_prev[:, span], v_prev[:, span]
        score_b = nt(q, kb) * scale + mask_prev[...]
        score = nt(q, k) * scale + mask_now[...]
        top = jnp.max(jnp.maximum(score, score_b), axis=1, keepdims=True)
        prob_b = jnp.exp(score_b - top)
        prob = jnp.exp(score - top)
        total = jnp.sum(prob + prob_b, axis=1, keepdims=True)
        inverse = 1.0 / total
        prob_b = prob_b * inverse
        prob = prob * inverse
        low_b, low = prob_b.astype(jnp.bfloat16), prob.astype(jnp.bfloat16)
        attended = (nn(low_b, vb) + nn(low, v)).astype(jnp.bfloat16)
        att_ref[:, span] = attended
        term = jnp.sum(
            do.astype(jnp.float32) * attended.astype(jnp.float32), axis=1, keepdims=True
        )
        stats[:, h : h + 1] = top + jnp.log(total)
        stats[:, heads + h : heads + h + 1] = term
        sg_b = (prob_b * (nt(do, vb) - term)).astype(jnp.bfloat16)
        sg = (prob * (nt(do, v) - term)).astype(jnp.bfloat16)
        qgrad_ref[:, span] = ((nn(sg_b, kb) + nn(sg, k)) * scale).astype(jnp.bfloat16)
        key_own[h] = tn(sg, q)
        value_own[h] = tn(low, do)

    def head_second(h):
        span = pl.ds(h * HD, HD)
        q, do, k, v = q_next[:, span], do_next[:, span], k_ref[:, span], v_ref[:, span]
        score = nt(q, k) * scale + mask_next[...]
        prob = jnp.exp(score - stats_next[:, h : h + 1])
        sg = prob * (nt(do, v) - stats_next[:, heads + h : heads + h + 1])
        key = key_own[h] + tn(sg.astype(jnp.bfloat16), q)
        kgrad_ref[:, span] = (key * scale).astype(jnp.bfloat16)
        value = value_own[h] + tn(prob.astype(jnp.bfloat16), do)
        vgrad_ref[:, span] = value.astype(jnp.bfloat16)

    hops = 1
    for h in range(heads):
        head_first(h)
        while hops < shards and hops * heads <= (h + 1) * (shards - 1):
            hop(hops)
            hops += 1

    @pl.when(z > 0)
    def _():
        stats_copy.start()

    def owner(b):
        return b % peers

    def rs_copy(b, sender, target):
        return pltpu.make_async_remote_copy(
            src_ref=red.at[b],
            dst_ref=rs_buf.at[b // peers, sender],
            send_sem=rs_send.at[b],
            recv_sem=rs_recv.at[b // peers, sender],
            device_id=at(target),
            device_id_type=MESH,
        )

    def ag_copy(b, target):
        return pltpu.make_async_remote_copy(
            src_ref=fin.at[b],
            dst_ref=fin.at[b],
            send_sem=ag_send.at[b // peers, target],
            recv_sem=ag_recv.at[b],
            device_id=at(target),
            device_id_type=MESH,
        )

    def second_pass(b, carry):
        lanes = lanes_of(b)
        start = state_in[:, lanes]
        later = adj_in[:, lanes]
        for j in range(SUB):
            rows = pl.ds(j, states, stride=SUB)
            fold[0, rows] = start
            start = ends[b, rows] + through[b, rows] * start
            rows = pl.ds(SUB - 1 - j, states, stride=SUB)
            fold[1, rows] = later
            later = leads[b, rows] + through[b, rows] * later
        skip = skip_ref[:, lanes]
        state = fold[0].reshape(states, SUB, LANES)
        for s in range(steps):
            rows = pl.ds(s * SUB, SUB)
            size = step[rows, lanes]
            value = xp[rows, lanes]
            weight = size * value
            decay = jnp.exp2(size[None] * rb[b])
            dec[s] = decay
            prev[s] = state
            state = decay * state + weight[None] * wb[0, s]
            mix_p[rows] = jnp.sum(state * wb[1, s], axis=0) + skip * value
        back = fold[1].reshape(states, SUB, LANES)
        accum = jnp.zeros((states, SUB, LANES), jnp.float32)
        for s in reversed(range(steps)):
            rows = pl.ds(s * SUB, SUB)
            size = step[rows, lanes]
            out = gp[rows, lanes]
            adjoint = wb[1, s] * out[None] + back
            through_write = jnp.sum(adjoint * wb[0, s], axis=0)
            back = dec[s] * adjoint
            tail = back * prev[s]
            xg_p[rows] = through_write * size + skip * out
            total = jnp.sum(tail * rb[b], axis=0) * LN2
            rg_p[rows] = (xp[rows, lanes] * through_write + total) * sig[rows, lanes]
            accum = accum + tail * size[None]
        fold[0] = accum.reshape(states * SUB, LANES)
        decay_sum = fold[0, pl.ds(0, states, stride=SUB)]
        for j in range(1, SUB):
            decay_sum = decay_sum + fold[0, pl.ds(j, states, stride=SUB)]
        red[b, pl.ds(0, states)] = decay_sum * rate2[:, lanes] * LN2
        skip_sum = jnp.sum(gp[:, lanes] * xp[:, lanes], axis=0, keepdims=True)
        bias_sum = jnp.sum(rg_p[...], axis=0, keepdims=True)
        which = lax.broadcasted_iota(jnp.int32, (RED_ROWS - states, LANES), 0)
        red[b, pl.ds(states, RED_ROWS - states)] = jnp.where(
            which == 0, skip_sum, jnp.where(which == 1, bias_sum, 0.0)
        )
        target = owner(b)

        @pl.when(target != me)
        def _():
            rs_copy(b, me, target).start()

        for source, out_ref in ((mix_p, mix_ref), (xg_p, xgrad_ref), (rg_p, rgrad_ref)):
            moved = nn(back_order, source[...].astype(jnp.bfloat16))
            out_ref[:, lanes] = moved.astype(jnp.bfloat16)
        return carry

    lax.fori_loop(0, blocks, second_pass, 0)

    @pl.when(z < shards - 1)
    def _():
        for copy in down:
            copy.wait_recv()
        stats_copy.wait_recv()

    docs_next = jnp.broadcast_to(doc_next[...].astype(jnp.float32), (length, length)).T
    docs_here = jnp.broadcast_to(doc_ref[...].astype(jnp.float32), (length, length))
    seen = (docs_next == docs_here) & (row < col) & (z < shards - 1)
    mask_next[...] = jnp.where(seen, 0.0, NEG)

    def finish(slot, carry):
        b = slot * peers + me

        @pl.when(b < blocks)
        def _():
            def gather(peer, total):
                @pl.when(peer != me)
                def _():
                    rs_copy(b, peer, peer).wait_recv()
                    fin[b] = fin[b] + rs_buf[slot, peer]

                return total

            fin[b] = red[b]
            lax.fori_loop(0, peers, gather, 0)

            def spread(peer, total):
                @pl.when(peer != me)
                def _():
                    ag_copy(b, peer).start()

                return total

            lax.fori_loop(0, peers, spread, 0)

        return carry

    for h in range(heads // 2):
        head_second(h)
    lax.fori_loop(0, slots, finish, 0)
    for h in range(heads // 2, heads):
        head_second(h)

    def collect(b, carry):
        @pl.when(owner(b) != me)
        def _():
            ag_copy(b, owner(b)).wait_recv()
            rs_copy(b, me, owner(b)).wait_send()

        @pl.when(owner(b) == me)
        def _():
            def sent(peer, total):
                @pl.when(peer != me)
                def _():
                    ag_copy(b, peer).wait_send()

                return total

            lax.fori_loop(0, peers, sent, 0)

        return carry

    lax.fori_loop(0, blocks, collect, 0)
    sums_ref[...] = fin[...] * (1.0 / math.sqrt(length * peers))

    @pl.when(z < shards - 1)
    def _():
        for copy in up + [state_copy]:
            copy.wait_send()

    @pl.when(z > 0)
    def _():
        for copy in down + [adj_copy, stats_copy]:
            copy.wait_send()


def body(
    mixer_in, delta_raw, delta_bias, decay_log, skip_gain, state_write, state_read, mixer_grad,
    attn_query, attn_key, attn_value, attn_grad, document_id,
):
    shards, copies = lax.axis_size("seq"), lax.axis_size("dp")
    peers = shards * copies
    length, channels = mixer_in.shape[1:]
    width = attn_query.shape[2]
    states = decay_log.shape[1]
    blocks = channels // LANES
    heads = width // HD
    steps = length // SUB
    slots = -(-blocks // peers)
    f32, bf16 = jnp.float32, jnp.bfloat16
    wide = pltpu.VMEM((length, channels), f32)
    rows = pltpu.VMEM((states, channels), f32)
    seg = pltpu.VMEM((blocks, states * SUB, LANES), f32)
    tile = pltpu.VMEM((length, LANES), f32)
    attn = pltpu.VMEM((length, width), bf16)
    doc = pltpu.VMEM((1, length), jnp.int32)
    square = pltpu.VMEM((length, length), f32)
    own = pltpu.VMEM((heads, length, HD), f32)
    dma = pltpu.SemaphoreType.DMA
    trail = pltpu.VMEM((steps, states, SUB, LANES), f32)
    outs = pl.pallas_call(
        functools.partial(kernel, shards, copies),
        out_shape=(
            [jax.ShapeDtypeStruct((length, channels), bf16)] * 3
            + [jax.ShapeDtypeStruct((blocks, RED_ROWS, LANES), f32)]
            + [jax.ShapeDtypeStruct((length, width), bf16)] * 4
        ),
        in_specs=[pl.BlockSpec(memory_space=pltpu.VMEM)] * 13,
        out_specs=[pl.BlockSpec(memory_space=pltpu.VMEM)] * 8,
        scratch_shapes=[
            wide, wide, wide, wide,
            pltpu.VMEM((2, steps, states, SUB, LANES), f32),
            pltpu.VMEM((blocks, states, SUB, LANES), f32),
            rows, seg, seg, seg,
            rows, rows, rows, rows, rows, rows, rows,
            trail, trail, pltpu.VMEM((2, states * SUB, LANES), f32), tile, tile, tile,
            attn, attn, attn, attn, doc, doc,
            tile, tile, own, own, square, square, square,
            pltpu.VMEM((blocks, RED_ROWS, LANES), f32),
            pltpu.VMEM((slots, peers, RED_ROWS, LANES), f32),
            pltpu.VMEM((blocks, RED_ROWS, LANES), f32),
            dma((7,)), dma((7,)), dma((2,)), dma((2,)),
            dma((blocks,)), dma((slots, peers)), dma((slots, peers)), dma((blocks,)),
        ],
        compiler_params=pltpu.CompilerParams(
            collective_id=0, has_side_effects=True, vmem_limit_bytes=60 * 1024 * 1024
        ),
    )(
        mixer_in[0], delta_raw[0], mixer_grad[0], delta_bias[None], decay_log.T, skip_gain[None],
        state_write[0], state_read[0], attn_query[0], attn_key[0], attn_value[0], attn_grad[0],
        document_id,
    )
    mixed, input_grad, delta_grad, sums, attended, query_grad, key_grad, value_grad = outs
    decay_grad = sums[:, :states].transpose(0, 2, 1).reshape(channels, states)
    return (
        mixed[None], input_grad[None], delta_grad[None], decay_grad,
        sums[:, states].reshape(channels), sums[:, states + 1].reshape(channels),
        attended[None], query_grad[None], key_grad[None], value_grad[None],
    )


def solution(mesh):
    sequence = P(("member", "dp"), "seq", "mp")
    shared = P(("member", "dp"), "seq", None)
    channel, table = P(("member", "mp")), P(("member", "mp"), None)
    return jax.shard_map(
        body,
        mesh=mesh,
        in_specs=(
            sequence, sequence, channel, table, channel, shared, shared, sequence,
            sequence, sequence, sequence, sequence, P(("member", "dp"), "seq"),
        ),
        out_specs=(
            sequence, sequence, sequence, table, channel, channel,
            sequence, sequence, sequence, sequence,
        ),
        check_vma=False,
    )
```

```python
import functools
import math

import jax
import jax.numpy as jnp
from jax import lax
from jax.experimental import pallas as pl
from jax.experimental.pallas import tpu as pltpu
from jax.sharding import PartitionSpec as P

HD = 96
WINDOW = 128
LANES = 128
SUB = 8
RED_ROWS = 24
LOG2E = math.log2(math.e)
LN2 = math.log(2.0)
NEG = -1e30
MESH = pl.DeviceIdType.MESH


def dot(a, b, contract):
    return lax.dot_general(a, b, (contract, ((), ())), preferred_element_type=jnp.float32)


def nn(a, b):
    return dot(a, b, ((1,), (0,)))


def nt(a, b):
    return dot(a, b, ((1,), (1,)))


def tn(a, b):
    return dot(a, b, ((0,), (0,)))


def kernel(
    shards,
    copies,
    x_ref, raw_ref, grad_ref, bias_ref, decay_ref, skip_ref, write_ref, read_ref,
    q_ref, k_ref, v_ref, do_ref, doc_ref,
    mix_ref, xgrad_ref, rgrad_ref, att_ref, qgrad_ref, kgrad_ref, vgrad_ref,
    decay_out, skip_out, bias_out,
    xp, gp, step, sig, wb, rb, rate2, ends, through, leads,
    dev_end, dev_through, dev_lead, state_in, adj_in, state_out, adj_out,
    dec, prev, fold, mix_p, xg_p, rg_p,
    k_prev, v_prev, q_next, do_next, doc_prev, doc_next,
    stats, stats_next, key_own, value_own, mask_prev, mask_now, mask_next,
    red, rs_buf, fin,
    near_send, near_recv, chain_send, chain_recv, rs_send, rs_recv, ag_send, ag_recv,
):
    z, dp = lax.axis_index("seq"), lax.axis_index("dp")
    peers = shards * copies
    me = dp * shards + z
    length, channels = x_ref.shape
    states = decay_ref.shape[0]
    blocks = channels // LANES
    steps = length // SUB
    heads = q_ref.shape[1] // HD
    slots = rs_buf.shape[0]

    def at(peer):
        return {"seq": peer % shards, "dp": peer // shards}

    barrier = pltpu.get_barrier_semaphore()

    def greet(peer, carry):
        @pl.when(peer != me)
        def _():
            pl.semaphore_signal(barrier, inc=1, device_id=at(peer), device_id_type=MESH)

        return carry

    lax.fori_loop(0, peers, greet, 0)
    pl.semaphore_wait(barrier, peers - 1)

    def near(index, src, dst, offset, sems=None):
        send, recv = sems or (near_send, near_recv)
        return pltpu.make_async_remote_copy(
            src_ref=src,
            dst_ref=dst,
            send_sem=send.at[index],
            recv_sem=recv.at[index],
            device_id={"seq": z + offset},
            device_id_type=MESH,
        )

    up = [near(0, doc_ref, doc_prev, 1), near(1, k_ref, k_prev, 1), near(2, v_ref, v_prev, 1)]
    down = [
        near(3, doc_ref, doc_next, -1),
        near(4, q_ref, q_next, -1),
        near(5, do_ref, do_next, -1),
    ]
    stats_copy = near(6, stats, stats_next, -1)
    chain = (chain_send, chain_recv)
    state_copy = near(0, state_out, state_in, 1, chain)
    adj_copy = near(1, adj_out, adj_in, -1, chain)

    @pl.when(z < shards - 1)
    def _():
        for copy in up:
            copy.start()

    @pl.when(z > 0)
    def _():
        for copy in down:
            copy.start()

    @pl.when(z == 0)
    def _():
        k_prev[...] = jnp.zeros_like(k_prev)
        v_prev[...] = jnp.zeros_like(v_prev)
        doc_prev[...] = jnp.zeros_like(doc_prev)
        state_in[...] = jnp.zeros_like(state_in)

    @pl.when(z == shards - 1)
    def _():
        q_next[...] = jnp.zeros_like(q_next)
        do_next[...] = jnp.zeros_like(do_next)
        doc_next[...] = jnp.zeros_like(doc_next)
        stats_next[...] = jnp.zeros_like(stats_next)
        adj_in[...] = jnp.zeros_like(adj_in)

    row = lax.broadcasted_iota(jnp.int32, (length, length), 0)
    col = lax.broadcasted_iota(jnp.int32, (length, length), 1)
    order = (col == steps * (row % SUB) + row // SUB).astype(jnp.float32).astype(jnp.bfloat16)
    back_order = (row == steps * (col % SUB) + col // SUB).astype(jnp.float32).astype(jnp.bfloat16)

    writes = nt(order, write_ref[...])
    reads = nt(order, read_ref[...])
    for n in range(states):
        wb[0, :, n] = jnp.broadcast_to(writes[:, n : n + 1], (length, LANES)).reshape(
            steps, SUB, LANES
        )
        wb[1, :, n] = jnp.broadcast_to(reads[:, n : n + 1], (length, LANES)).reshape(
            steps, SUB, LANES
        )
    rate2[...] = -jnp.exp(decay_ref[...]) * LOG2E

    def lanes_of(b):
        return pl.ds(pl.multiple_of(b * LANES, LANES), LANES)

    half = states // 2

    def first_pass(b, carry):
        lanes = lanes_of(b)
        xp[:, lanes] = nn(order, x_ref[:, lanes])
        gp[:, lanes] = nn(order, grad_ref[:, lanes])
        arg = nn(order, raw_ref[:, lanes]) + bias_ref[pl.ds(b, 1)]
        small = jnp.exp(-jnp.abs(arg))
        step[:, lanes] = jnp.maximum(arg, 0.0) + jnp.log(1.0 + small)
        sig[:, lanes] = jnp.where(arg >= 0.0, 1.0, small) / (1.0 + small)
        rates = rate2[:, lanes]
        for n in range(states):
            rb[b, n] = jnp.broadcast_to(rates[n : n + 1], (SUB, LANES))
        for part in range(2):
            some = pl.ds(part * half, half)
            rate = rb[b, some]
            state = jnp.zeros((half, SUB, LANES), jnp.float32)
            lead = jnp.zeros((half, SUB, LANES), jnp.float32)
            product = None
            for s in range(steps):
                rows = pl.ds(s * SUB, SUB)
                size = step[rows, lanes]
                weight = size * xp[rows, lanes]
                decay = jnp.exp2(size[None] * rate)
                state = decay * state + weight[None] * wb[0, s, some]
                product = decay if product is None else product * decay
                lead = lead + product * (gp[rows, lanes][None] * wb[1, s, some])
            flat = pl.ds(part * half * SUB, half * SUB)
            ends[b, flat] = state.reshape(half * SUB, LANES)
            through[b, flat] = product.reshape(half * SUB, LANES)
            leads[b, flat] = lead.reshape(half * SUB, LANES)
        end = jnp.zeros((states, LANES), jnp.float32)
        lead = jnp.zeros((states, LANES), jnp.float32)
        total = jnp.ones((states, LANES), jnp.float32)
        for j in range(SUB):
            rows = pl.ds(j, states, stride=SUB)
            now = through[b, rows]
            end = ends[b, rows] + now * end
            total = total * now
            rows = pl.ds(SUB - 1 - j, states, stride=SUB)
            lead = leads[b, rows] + through[b, rows] * lead
        dev_end[:, lanes] = end
        dev_lead[:, lanes] = lead
        dev_through[:, lanes] = total
        return carry

    lax.fori_loop(0, blocks, first_pass, 0)

    def hop(k):
        @pl.when(z == k)
        def _():
            if k > 0:
                state_copy.wait_recv()
            if k < shards - 1:
                state_out[...] = dev_end[...] + dev_through[...] * state_in[...]
                state_copy.start()

        @pl.when(z == shards - 1 - k)
        def _():
            if k > 0:
                adj_copy.wait_recv()
            if k < shards - 1:
                adj_out[...] = dev_lead[...] + dev_through[...] * adj_in[...]
                adj_copy.start()

    hop(0)

    @pl.when(z > 0)
    def _():
        for copy in up:
            copy.wait_recv()

    docs_now = jnp.broadcast_to(doc_ref[...].astype(jnp.float32), (length, length))
    docs_prev = jnp.broadcast_to(doc_prev[...].astype(jnp.float32), (length, length))
    docs_own = docs_now.T
    seen = (docs_now == docs_own) & (row >= col)
    mask_now[...] = jnp.where(seen, 0.0, NEG)
    seen = (docs_prev == docs_own) & (row < col) & (z > 0)
    mask_prev[...] = jnp.where(seen, 0.0, NEG)
    scale = 1.0 / math.sqrt(HD)

    def head_first(h):
        span = pl.ds(h * HD, HD)
        q, k, v, do = q_ref[:, span], k_ref[:, span], v_ref[:, span], do_ref[:, span]
        kb, vb = k_prev[:, span], v_prev[:, span]
        score_b = nt(q, kb) * scale + mask_prev[...]
        score = nt(q, k) * scale + mask_now[...]
        top = jnp.max(jnp.maximum(score, score_b), axis=1, keepdims=True)
        prob_b = jnp.exp(score_b - top)
        prob = jnp.exp(score - top)
        total = jnp.sum(prob + prob_b, axis=1, keepdims=True)
        inverse = 1.0 / total
        prob_b = prob_b * inverse
        prob = prob * inverse
        low_b, low = prob_b.astype(jnp.bfloat16), prob.astype(jnp.bfloat16)
        attended = (nn(low_b, vb) + nn(low, v)).astype(jnp.bfloat16)
        att_ref[:, span] = attended
        term = jnp.sum(
            do.astype(jnp.float32) * attended.astype(jnp.float32), axis=1, keepdims=True
        )
        stats[:, h : h + 1] = top + jnp.log(total)
        stats[:, heads + h : heads + h + 1] = term
        sg_b = (prob_b * (nt(do, vb) - term)).astype(jnp.bfloat16)
        sg = (prob * (nt(do, v) - term)).astype(jnp.bfloat16)
        qgrad_ref[:, span] = ((nn(sg_b, kb) + nn(sg, k)) * scale).astype(jnp.bfloat16)
        key_own[h] = tn(sg, q)
        value_own[h] = tn(low, do)

    def head_second(h):
        span = pl.ds(h * HD, HD)
        q, do, k, v = q_next[:, span], do_next[:, span], k_ref[:, span], v_ref[:, span]
        score = nt(q, k) * scale + mask_next[...]
        prob = jnp.exp(score - stats_next[:, h : h + 1])
        sg = prob * (nt(do, v) - stats_next[:, heads + h : heads + h + 1])
        key = key_own[h] + tn(sg.astype(jnp.bfloat16), q)
        kgrad_ref[:, span] = (key * scale).astype(jnp.bfloat16)
        value = value_own[h] + tn(prob.astype(jnp.bfloat16), do)
        vgrad_ref[:, span] = value.astype(jnp.bfloat16)

    hops = 1
    for h in range(heads):
        head_first(h)
        while hops < shards and hops * heads <= (h + 1) * (shards - 1):
            hop(hops)
            hops += 1

    @pl.when(z > 0)
    def _():
        stats_copy.start()

    def owner(b):
        return b % peers

    def rs_copy(b, sender, target):
        return pltpu.make_async_remote_copy(
            src_ref=red.at[b],
            dst_ref=rs_buf.at[b // peers, sender],
            send_sem=rs_send.at[b],
            recv_sem=rs_recv.at[b // peers, sender],
            device_id=at(target),
            device_id_type=MESH,
        )

    def ag_copy(b, target):
        return pltpu.make_async_remote_copy(
            src_ref=fin.at[b],
            dst_ref=fin.at[b],
            send_sem=ag_send.at[b // peers, target],
            recv_sem=ag_recv.at[b],
            device_id=at(target),
            device_id_type=MESH,
        )

    def second_pass(b, carry):
        lanes = lanes_of(b)
        start = state_in[:, lanes]
        later = adj_in[:, lanes]
        for j in range(SUB):
            rows = pl.ds(j, states, stride=SUB)
            fold[0, rows] = start
            start = ends[b, rows] + through[b, rows] * start
            rows = pl.ds(SUB - 1 - j, states, stride=SUB)
            fold[1, rows] = later
            later = leads[b, rows] + through[b, rows] * later
        skip = skip_ref[pl.ds(b, 1)]
        accums = []
        for part in range(2):
            some = pl.ds(part * half, half)
            flat = pl.ds(part * half * SUB, half * SUB)
            rate = rb[b, some]
            state = fold[0, flat].reshape(half, SUB, LANES)
            for s in range(steps):
                rows = pl.ds(s * SUB, SUB)
                size = step[rows, lanes]
                value = xp[rows, lanes]
                weight = size * value
                decay = jnp.exp2(size[None] * rate)
                dec[s, some] = decay
                prev[s, some] = state
                state = decay * state + weight[None] * wb[0, s, some]
                base = skip * value if part == 0 else mix_p[rows]
                mix_p[rows] = base + jnp.sum(state * wb[1, s, some], axis=0)
            back = fold[1, flat].reshape(half, SUB, LANES)
            accum = jnp.zeros((half, SUB, LANES), jnp.float32)
            for s in reversed(range(steps)):
                rows = pl.ds(s * SUB, SUB)
                size = step[rows, lanes]
                out = gp[rows, lanes]
                adjoint = wb[1, s, some] * out[None] + back
                through_write = jnp.sum(adjoint * wb[0, s, some], axis=0)
                back = dec[s, some] * adjoint
                tail = back * prev[s, some]
                total = jnp.sum(tail * rate, axis=0)
                if part == 0:
                    xg_p[rows] = through_write
                    rg_p[rows] = total
                else:
                    through_write = through_write + xg_p[rows]
                    total = (total + rg_p[rows]) * LN2
                    xg_p[rows] = through_write * size + skip * out
                    rg_p[rows] = (xp[rows, lanes] * through_write + total) * sig[rows, lanes]
                accum = accum + tail * size[None]
            accums.append(accum)
        accum = jnp.concatenate(accums, axis=0)
        fold[0] = accum.reshape(states * SUB, LANES)
        decay_sum = fold[0, pl.ds(0, states, stride=SUB)]
        for j in range(1, SUB):
            decay_sum = decay_sum + fold[0, pl.ds(j, states, stride=SUB)]
        red[b, pl.ds(0, states)] = decay_sum * rate2[:, lanes] * LN2
        skip_sum = jnp.sum(gp[:, lanes] * xp[:, lanes], axis=0, keepdims=True)
        bias_sum = jnp.sum(rg_p[...], axis=0, keepdims=True)
        which = lax.broadcasted_iota(jnp.int32, (RED_ROWS - states, LANES), 0)
        red[b, pl.ds(states, RED_ROWS - states)] = jnp.where(
            which == 0, skip_sum, jnp.where(which == 1, bias_sum, 0.0)
        )
        target = owner(b)

        @pl.when(target != me)
        def _():
            rs_copy(b, me, target).start()

        for source, out_ref in ((mix_p, mix_ref), (xg_p, xgrad_ref), (rg_p, rgrad_ref)):
            moved = nn(back_order, source[...].astype(jnp.bfloat16))
            out_ref[:, lanes] = moved.astype(jnp.bfloat16)
        return carry

    lax.fori_loop(0, blocks, second_pass, 0)

    @pl.when(z < shards - 1)
    def _():
        for copy in down:
            copy.wait_recv()
        stats_copy.wait_recv()

    docs_next = jnp.broadcast_to(doc_next[...].astype(jnp.float32), (length, length)).T
    docs_here = jnp.broadcast_to(doc_ref[...].astype(jnp.float32), (length, length))
    seen = (docs_next == docs_here) & (row < col) & (z < shards - 1)
    mask_next[...] = jnp.where(seen, 0.0, NEG)

    def finish(slot, carry):
        b = slot * peers + me

        @pl.when(b < blocks)
        def _():
            def gather(peer, total):
                @pl.when(peer != me)
                def _():
                    rs_copy(b, peer, peer).wait_recv()
                    fin[b] = fin[b] + rs_buf[slot, peer]

                return total

            fin[b] = red[b]
            lax.fori_loop(0, peers, gather, 0)

            def spread(peer, total):
                @pl.when(peer != me)
                def _():
                    ag_copy(b, peer).start()

                return total

            lax.fori_loop(0, peers, spread, 0)

        return carry

    for h in range(heads // 2):
        head_second(h)
    lax.fori_loop(0, slots, finish, 0)
    for h in range(heads // 2, heads):
        head_second(h)

    def collect(b, carry):
        @pl.when(owner(b) != me)
        def _():
            ag_copy(b, owner(b)).wait_recv()
            rs_copy(b, me, owner(b)).wait_send()

        @pl.when(owner(b) == me)
        def _():
            def sent(peer, total):
                @pl.when(peer != me)
                def _():
                    ag_copy(b, peer).wait_send()

                return total

            lax.fori_loop(0, peers, sent, 0)

        return carry

    lax.fori_loop(0, blocks, collect, 0)
    grad_scale = 1.0 / math.sqrt(length * peers)
    for b in range(blocks):
        summed = fin[b] * grad_scale
        decay_out[:, b * LANES : (b + 1) * LANES] = summed[:states]
        skip_out[b : b + 1] = summed[states : states + 1]
        bias_out[b : b + 1] = summed[states + 1 : states + 2]

    @pl.when(z < shards - 1)
    def _():
        for copy in up + [state_copy]:
            copy.wait_send()

    @pl.when(z > 0)
    def _():
        for copy in down + [adj_copy, stats_copy]:
            copy.wait_send()


def hand_over(*refs):
    count = (len(refs) - 2) // 3
    sources, targets, tiles = refs[:count], refs[count : 2 * count], refs[2 * count : 3 * count]
    in_sem, out_sem = refs[3 * count :]
    loads = [
        pltpu.make_async_copy(sources[i], tiles[i], in_sem.at[i]) for i in range(count)
    ]
    saves = [
        pltpu.make_async_copy(tiles[i], targets[i], out_sem.at[i]) for i in range(count)
    ]
    for load in loads:
        load.start()
    for load, save in zip(loads, saves):
        load.wait()
        save.start()
    for save in saves:
        save.wait()


def body(
    mixer_in, delta_raw, delta_bias, decay_log, skip_gain, state_write, state_read, mixer_grad,
    attn_query, attn_key, attn_value, attn_grad, document_id,
):
    shards, copies = lax.axis_size("seq"), lax.axis_size("dp")
    peers = shards * copies
    length, channels = mixer_in.shape[1:]
    width = attn_query.shape[2]
    states = decay_log.shape[1]
    blocks = channels // LANES
    heads = width // HD
    steps = length // SUB
    slots = -(-blocks // peers)
    f32, bf16 = jnp.float32, jnp.bfloat16
    wide = pltpu.VMEM((length, channels), f32)
    rows = pltpu.VMEM((states, channels), f32)
    seg = pltpu.VMEM((blocks, states * SUB, LANES), f32)
    tile = pltpu.VMEM((length, LANES), f32)
    attn = pltpu.VMEM((length, width), bf16)
    doc = pltpu.VMEM((1, length), jnp.int32)
    square = pltpu.VMEM((length, length), f32)
    own = pltpu.VMEM((heads, length, HD), f32)
    dma = pltpu.SemaphoreType.DMA
    trail = pltpu.VMEM((steps, states, SUB, LANES), f32)
    outs = pl.pallas_call(
        functools.partial(kernel, shards, copies),
        out_shape=(
            [jax.ShapeDtypeStruct((length, channels), bf16)] * 3
            + [jax.ShapeDtypeStruct((length, width), bf16)] * 4
            + [jax.ShapeDtypeStruct((states, channels), f32)]
            + [jax.ShapeDtypeStruct((blocks, LANES), f32)] * 2
        ),
        in_specs=[pl.BlockSpec(memory_space=pltpu.VMEM)] * 13,
        out_specs=[pl.BlockSpec(memory_space=pltpu.VMEM)] * 10,
        scratch_shapes=[
            wide, wide, wide, wide,
            pltpu.VMEM((2, steps, states, SUB, LANES), f32),
            pltpu.VMEM((blocks, states, SUB, LANES), f32),
            rows, seg, seg, seg,
            rows, rows, rows, rows, rows, rows, rows,
            trail, trail, pltpu.VMEM((2, states * SUB, LANES), f32), tile, tile, tile,
            attn, attn, attn, attn, doc, doc,
            tile, tile, own, own, square, square, square,
            pltpu.VMEM((blocks, RED_ROWS, LANES), f32),
            pltpu.VMEM((slots, peers, RED_ROWS, LANES), f32),
            pltpu.VMEM((blocks, RED_ROWS, LANES), f32),
            dma((7,)), dma((7,)), dma((2,)), dma((2,)),
            dma((blocks,)), dma((slots, peers)), dma((slots, peers)), dma((blocks,)),
        ],
        compiler_params=pltpu.CompilerParams(
            collective_id=0, has_side_effects=True, vmem_limit_bytes=60 * 1024 * 1024
        ),
    )(
        mixer_in[0], delta_raw[0], mixer_grad[0], delta_bias.reshape(blocks, LANES),
        decay_log.T, skip_gain.reshape(blocks, LANES),
        state_write[0].T, state_read[0].T, attn_query[0], attn_key[0], attn_value[0], attn_grad[0],
        document_id,
    )
    count = len(outs)
    anywhere = [pl.BlockSpec(memory_space=pl.ANY)] * count
    outs = pl.pallas_call(
        hand_over,
        out_shape=[jax.ShapeDtypeStruct(o.shape, o.dtype) for o in outs],
        in_specs=anywhere,
        out_specs=anywhere,
        scratch_shapes=[pltpu.VMEM(o.shape, o.dtype) for o in outs]
        + [dma((count,)), dma((count,))],
    )(*outs)
    mixed, input_grad, delta_grad, attended, query_grad, key_grad, value_grad = outs[:7]
    decay_grad, skip_grad, bias_grad = outs[7:]
    return (
        mixed[None], input_grad[None], delta_grad[None], decay_grad.T,
        skip_grad.reshape(channels), bias_grad.reshape(channels),
        attended[None], query_grad[None], key_grad[None], value_grad[None],
    )


def solution(mesh):
    sequence = P(("member", "dp"), "seq", "mp")
    shared = P(("member", "dp"), "seq", None)
    channel, table = P(("member", "mp")), P(("member", "mp"), None)
    return jax.shard_map(
        body,
        mesh=mesh,
        in_specs=(
            sequence, sequence, channel, table, channel, shared, shared, sequence,
            sequence, sequence, sequence, sequence, P(("member", "dp"), "seq"),
        ),
        out_specs=(
            sequence, sequence, sequence, table, channel, channel,
            sequence, sequence, sequence, sequence,
        ),
        check_vma=False,
    )
```
